32 devices in a mesh: dp: 4 (over x, core), tensor: 8 (over z, y).
Axes of the slice: x: 2, y: 2, z: 4, core: 2. Of those that a mesh axis runs over, the one named last changes fastest.
Arguments:
- grad_out: bfloat16 [256, 4096], P(('dp', 'tensor')), may hold values from -6 to 6
- gate_pre: bfloat16 [256, 14848], P('dp', 'tensor'), may hold values from -8 to 8
- up_pre: bfloat16 [256, 14848], P('dp', 'tensor'), may hold values from -6 to 6
- down_weight: bfloat16 [4096, 14848], P(None, 'tensor'), may hold values from -1.5 to 1.5
Outputs:
- grad_weight: float32 [4096, 14848], P('dp', 'tensor')
- grad_gate: bfloat16 [256, 14848], P('dp', 'tensor')
- grad_up: bfloat16 [256, 14848], P('dp', 'tensor')
The draws below stay inside these ranges and needn't reach their ends.
All inputs are finite; a program needn't handle non-finite values.
Results may differ from the reference program's by a relative error of at most 0.015.
Values may be sent and summed in bfloat16 or wider, within the bound.
A program may use at most 128 MiB of HBM per device.

```python
import jax
import jax.numpy as jnp
from jax import lax

D_W = 4096
FF_W = 14848
TOKG = 64
TOKENS = 256
N_DP = 4


def raised(array, key, source, target, blocks, factor):
    def block_of(dim):
        return (jnp.arange(array.shape[dim]) // (array.shape[dim] // blocks)).reshape((-1,) + (1,) * (array.ndim - 1 - dim))

    near = jax.random.permutation(key, blocks)[block_of(target)]
    far = (block_of(target) + blocks // 2) % blocks
    return jnp.where((block_of(source) == near) | (block_of(source) == far), factor * array, array)


def shard_levels(own_key, shape, cuts, low, high):
    def one(dim, parts):
        draws = jax.random.uniform(jax.random.fold_in(jax.random.fold_in(own_key, 6), dim), (parts,), jnp.float32, low / len(cuts), high / len(cuts))
        return jnp.repeat(jnp.exp(draws), shape[dim] // parts).reshape((-1,) + (1,) * (len(shape) - dim - 1))

    loudness = one(*cuts[0])
    for cut in cuts[1:]:
        loudness = loudness * one(*cut)
    return loudness


def normal_values(rng, shape, scale, bound, split=(), held_as=jnp.bfloat16):
    array = jax.random.normal(rng, shape, jnp.float32) * scale
    if len(split) > 0:
        array = shard_levels(rng, shape, split, -0.22, 0.18) * array
    return jnp.clip(array, min=-bound, max=bound).astype(held_as)


def gaussian_with(stream_key, dims, width, most, shards, heavy, kind=jnp.bfloat16):
    values = width * jax.random.normal(stream_key, dims, jnp.float32)
    if shards:
        values = values * shard_levels(stream_key, dims, shards, -0.22, 0.18)
    return jnp.clip(raised(values, jax.random.fold_in(stream_key, 3), *heavy), -most, most).astype(kind)


def setup_inputs(seed: int = 0) -> dict:
    seeds = jax.random.split(jax.random.key(seed), 5)
    grad_out = gaussian_with(seeds[0], (TOKENS, D_W), (4 * TOKENS ** -0.5), 6.0, ((0, 32),), (0, 1, 32, 2.75))
    gate_pre = normal_values(seeds[1], (TOKENS, FF_W), 2.0, 8.0, ((0, 4), (1, 8)))
    up_pre = normal_values(seeds[2], (TOKENS, FF_W), 1.0, 6.0, ((0, 4), (1, 8)))
    down_weight = normal_values(seeds[3], (D_W, FF_W), (max(D_W // 256, 1)) ** -0.5, 1.5, ((1, 8),))
    return dict(grad_out=grad_out, gate_pre=gate_pre, up_pre=up_pre, down_weight=down_weight)


def reference(grad_out, gate_pre, up_pre, down_weight):
    gate = gate_pre.astype(jnp.float32)
    upper = up_pre.astype(jnp.float32)
    sig = jax.nn.sigmoid(gate)
    act = gate * sig
    hidden = (act * upper).astype(jnp.bfloat16)
    grad_hidden = jnp.dot(grad_out, down_weight, preferred_element_type=jnp.float32)
    grad_up = (grad_hidden * act).astype(jnp.bfloat16)
    grad_gate = (grad_hidden * upper * sig * (1.0 + gate * (1.0 - sig))).astype(jnp.bfloat16)
    grouped_out = grad_out.reshape(N_DP, TOKG, D_W)
    grouped_hidden = hidden.reshape(N_DP, TOKG, FF_W)

    def add_group(total, pair):
        part = jnp.dot(pair[0].T, pair[1], preferred_element_type=jnp.float32)
        rounded = lax.optimization_barrier(part.astype(jnp.bfloat16))
        return total + rounded.astype(jnp.float32), None

    grad_weight, unused = lax.scan(add_group, jnp.zeros((D_W, FF_W), jnp.float32), (grouped_out, grouped_hidden))
    return grad_weight, grad_gate, grad_up
```

```python
import functools

import jax
import jax.numpy as jnp
from jax import lax
from jax.experimental import pallas as pl
from jax.experimental.pallas import tpu as pltpu
from jax.sharding import PartitionSpec as P

MESH = pl.DeviceIdType.MESH
CORES = 2


def gather_kernel(
    n_dp, n_t, outer, widths,
    go_hbm, gate_hbm, up_hbm, weight_hbm,
    cols_ref, hidden_ref, grad_ref,
    rows, gate, upper, weight, left,
    load_sem, weight_sem, send_sem,
    rows_sem, cross_sem, line_sem, hidden_sem, pair_sem,
):
    inner = n_t // outer
    n_chip = n_dp // CORES
    depth = go_hbm.shape[0]
    feats = cols_ref.shape[-1]
    dp, t = lax.axis_index("dp"), lax.axis_index("tensor")
    chip, core = dp // CORES, dp % CORES
    mate = chip * CORES + (1 - core)
    a, b = t // inner, t % inner
    chips = [lax.rem(chip + d, n_chip) for d in range(1, n_chip)]
    lines = [lax.rem(a + d, outer) * inner + b for d in range(1, outer)]
    sides = [a * inner + lax.rem(b + d, inner) for d in range(1, inner)]

    loads = [
        pltpu.make_async_copy(go_hbm, rows.at[t], load_sem.at[0]),
        pltpu.make_async_copy(gate_hbm, gate, load_sem.at[1]),
        pltpu.make_async_copy(up_hbm, upper, load_sem.at[2]),
    ]
    for load in loads:
        load.start()
    weight_loads = []
    start = 0
    for k, width in enumerate(widths):
        span = pl.ds(start, width)
        weight_loads.append(pltpu.make_async_copy(weight_hbm.at[:, span], weight.at[:, span], weight_sem.at[k]))
        weight_loads[-1].start()
        start += width

    barrier = pltpu.get_barrier_semaphore()
    peers = [(lax.rem(dp + d, n_dp), t) for d in range(1, n_dp)]
    peers += [(dp, other) for other in lines + sides]
    for peer in peers:
        pl.semaphore_signal(barrier, inc=1, device_id=peer, device_id_type=MESH)
    loads[0].wait()
    pl.semaphore_wait(barrier, len(peers))

    sent = []

    def send(src, dst, sem, peer):
        copy = pltpu.make_async_remote_copy(
            src_ref=src, dst_ref=dst, send_sem=send_sem.at[len(sent)], recv_sem=sem,
            device_id=peer, device_id_type=MESH,
        )
        copy.start()
        sent.append(copy)

    def arrived(dst, sem):
        pltpu.make_async_remote_copy(
            src_ref=dst, dst_ref=dst, send_sem=send_sem.at[0], recv_sem=sem,
            device_id=(mate, t), device_id_type=MESH,
        ).wait_recv()

    def block_of(group):
        return pl.ds(pl.multiple_of(group * feats, feats), feats)

    for other in chips:
        for c in range(CORES):
            group = other * CORES + c
            send(rows.at[t, :, block_of(group)], cols_ref.at[chip, core, t], cross_sem.at[chip, core], (group, t))
    for peer in lines + sides:
        send(rows.at[t], rows.at[t], rows_sem.at[t], (dp, peer))

    loads[1].wait()
    loads[2].wait()
    g = gate[...].astype(jnp.float32)
    u = upper[...].astype(jnp.float32)
    hidden_ref[chip, core] = (g * jax.nn.sigmoid(g) * u).astype(jnp.bfloat16)
    mine = hidden_ref.at[chip, core]
    for other in chips:
        send(mine, mine, hidden_sem.at[chip, core], (other * CORES + core, t))
    send(mine, mine, hidden_sem.at[chip, core], (mate, t))

    for other in chips:
        for c in range(CORES):
            arrived(cols_ref.at[other, c, t], cross_sem.at[other, c])
        block = cols_ref.at[other, :, t]
        for peer in lines + sides:
            send(block, block, line_sem.at[other, t], (dp, peer))

    for source in lines:
        arrived(rows.at[source], rows_sem.at[source])
        for side in sides:
            send(rows.at[source], rows.at[source], rows_sem.at[source], (dp, side))
    for source in lines:
        for other in chips:
            block = cols_ref.at[other, :, source]
            arrived(block, line_sem.at[other, source])
            for side in sides:
                send(block, block, line_sem.at[other, source], (dp, side))

    for other in chips:
        block = hidden_ref.at[other, core]
        arrived(block, hidden_sem.at[other, core])
        send(block, block, hidden_sem.at[other, core], (mate, t))

    from_sides = [
        step * inner + lax.rem(b + d, inner)
        for step in range(outer) for d in range(1, inner)
    ]
    for source in from_sides:
        arrived(rows.at[source], rows_sem.at[source])
    send(rows.at[:, :, block_of(mate)], cols_ref.at[chip, core], pair_sem.at[0], (mate, t))
    keep = pltpu.make_async_copy(rows.at[:, :, block_of(dp)], cols_ref.at[chip, core], load_sem.at[3])
    keep.start()

    left[...] = rows[...].astype(jnp.float32).reshape(n_t * depth, -1).astype(jnp.bfloat16)
    start = 0
    for k, width in enumerate(widths):
        weight_loads[k].wait()
        span = pl.ds(start, width)
        grad_ref[:, span] = jnp.dot(left[...], weight[:, span], preferred_element_type=jnp.float32)
        start += width

    for source in from_sides:
        for other in chips:
            arrived(cols_ref.at[other, :, source], line_sem.at[other, source])
    for other in chips + [chip]:
        arrived(hidden_ref.at[other, 1 - core], hidden_sem.at[other, 1 - core])
    arrived(cols_ref.at[chip, 1 - core], pair_sem.at[0])
    keep.wait()
    for copy in sent:
        copy.wait_send()


def finish_kernel(cols_ref, hidden_ref, grad_ref, gate_ref, up_ref, weight_out, gate_out, up_out):
    weight_out[...] = lax.dot_general(
        cols_ref[...], hidden_ref[...], (((0,), (0,)), ((), ())), preferred_element_type=jnp.float32
    )
    grad = grad_ref[...]
    gate = gate_ref[...].astype(jnp.float32)
    upper = up_ref[...].astype(jnp.float32)
    sig = jax.nn.sigmoid(gate)
    up_out[...] = (grad * (gate * sig)).astype(jnp.bfloat16)
    gate_out[...] = (grad * upper * sig * (1.0 + gate * (1.0 - sig))).astype(jnp.bfloat16)


def body(n_dp, n_t, grad_out, gate_pre, up_pre, down_weight):
    depth, model = grad_out.shape
    group, wide = gate_pre.shape
    feats = model // n_dp
    n_chip = n_dp // CORES
    outer = 4 if n_t % 4 == 0 else 1
    inner = n_t // outer
    step = 512
    widths = [min(step, wide - start) for start in range(0, wide, step)]
    n_send = (
        (n_chip - 1) * CORES + (outer + inner - 2) * n_chip + n_chip
        + (outer - 1) * (inner - 1) * n_chip + n_chip + 1
    )
    anywhere = pl.BlockSpec(memory_space=pl.ANY)
    vmem = pl.BlockSpec(memory_space=pltpu.VMEM)
    dma = pltpu.SemaphoreType.DMA
    cols, hidden, grad = pl.pallas_call(
        functools.partial(gather_kernel, n_dp, n_t, outer, widths),
        out_shape=[
            jax.ShapeDtypeStruct((n_chip, CORES, n_t, depth, feats), jnp.bfloat16),
            jax.ShapeDtypeStruct((n_chip, CORES, group, wide), jnp.bfloat16),
            jax.ShapeDtypeStruct((group, wide), jnp.float32),
        ],
        in_specs=[anywhere] * 4,
        out_specs=[vmem] * 3,
        scratch_shapes=[
            pltpu.VMEM((n_t, depth, model), jnp.bfloat16),
            pltpu.VMEM((group, wide), jnp.bfloat16),
            pltpu.VMEM((group, wide), jnp.bfloat16),
            pltpu.VMEM((model, wide), jnp.bfloat16),
            pltpu.VMEM((group, model), jnp.bfloat16),
            dma((4,)),
            dma((len(widths),)),
            dma((n_send,)),
            dma((n_t,)),
            dma((n_chip, CORES)),
            dma((n_chip, n_t)),
            dma((n_chip, CORES)),
            dma((1,)),
        ],
        compiler_params=pltpu.CompilerParams(
            collective_id=0, has_side_effects=True, vmem_limit_bytes=48 * 1024 * 1024
        ),
    )(grad_out, gate_pre, up_pre, down_weight)
    cols = cols.reshape(n_dp * group, feats)
    hidden = hidden.reshape(n_dp * group, wide)

    tile = 128 if feats % 128 == 0 else feats
    steps = feats // tile
    while group % (steps * 16) != 0:
        tile, steps = tile * 2, steps // 2
    part = group // steps
    rows = pl.BlockSpec((part, wide), lambda i: (i, 0))
    return pl.pallas_call(
        finish_kernel,
        grid=(steps,),
        out_shape=[
            jax.ShapeDtypeStruct((feats, wide), jnp.float32),
            jax.ShapeDtypeStruct((group, wide), jnp.bfloat16),
            jax.ShapeDtypeStruct((group, wide), jnp.bfloat16),
        ],
        in_specs=[
            pl.BlockSpec((n_dp * group, tile), lambda i: (0, i)),
            pl.BlockSpec((n_dp * group, wide), lambda i: (0, 0)),
            rows, rows, rows,
        ],
        out_specs=[pl.BlockSpec((tile, wide), lambda i: (i, 0)), rows, rows],
        compiler_params=pltpu.CompilerParams(vmem_limit_bytes=48 * 1024 * 1024),
    )(cols, hidden, grad, gate_pre, up_pre)


def solution(mesh):
    in_specs = (P(("dp", "tensor"), None), P("dp", "tensor"), P("dp", "tensor"), P(None, "tensor"))
    out_specs = (P("dp", "tensor"), P("dp", "tensor"), P("dp", "tensor"))
    fn = functools.partial(body, mesh.shape["dp"], mesh.shape["tensor"])
    return jax.shard_map(fn, mesh=mesh, in_specs=in_specs, out_specs=out_specs, check_vma=False)
```

```python
import functools

import jax
import jax.numpy as jnp
from jax import lax
from jax.experimental import pallas as pl
from jax.experimental.pallas import tpu as pltpu
from jax.sharding import PartitionSpec as P

MESH = pl.DeviceIdType.MESH
CORES = 2


def gather_kernel(
    n_dp, n_t, outer, widths,
    go_hbm, gate_hbm, up_hbm, weight_hbm,
    cols_ref, hidden_ref, grad_ref,
    rows, gate, upper, weight, left,
    load_sem, weight_sem, send_sem,
    rows_sem, cross_sem, line_sem, hidden_sem, pair_sem,
):
    inner = n_t // outer
    n_chip = n_dp // CORES
    depth = go_hbm.shape[0]
    feats = cols_ref.shape[-1]
    dp, t = lax.axis_index("dp"), lax.axis_index("tensor")
    chip, core = dp // CORES, dp % CORES
    mate = chip * CORES + (1 - core)
    a, b = t // inner, t % inner
    chips = [lax.rem(chip + d, n_chip) for d in range(1, n_chip)]
    lines = [lax.rem(a + d, outer) * inner + b for d in range(1, outer)]
    sides = [a * inner + lax.rem(b + d, inner) for d in range(1, inner)]

    loads = [
        pltpu.make_async_copy(go_hbm, rows.at[t], load_sem.at[0]),
        pltpu.make_async_copy(gate_hbm, gate, load_sem.at[1]),
        pltpu.make_async_copy(up_hbm, upper, load_sem.at[2]),
    ]
    for load in loads:
        load.start()
    weight_loads = []
    start = 0
    for k, width in enumerate(widths):
        span = pl.ds(start, width)
        weight_loads.append(pltpu.make_async_copy(weight_hbm.at[span], weight.at[span], weight_sem.at[k]))
        weight_loads[-1].start()
        start += width

    barrier = pltpu.get_barrier_semaphore()
    peers = [(lax.rem(dp + d, n_dp), t) for d in range(1, n_dp)]
    peers += [(dp, other) for other in lines + sides]
    for peer in peers:
        pl.semaphore_signal(barrier, inc=1, device_id=peer, device_id_type=MESH)
    loads[0].wait()
    pl.semaphore_wait(barrier, len(peers))

    sent = []

    def send(src, dst, sem, peer):
        copy = pltpu.make_async_remote_copy(
            src_ref=src, dst_ref=dst, send_sem=send_sem.at[len(sent)], recv_sem=sem,
            device_id=peer, device_id_type=MESH,
        )
        copy.start()
        sent.append(copy)

    def arrived(dst, sem):
        pltpu.make_async_remote_copy(
            src_ref=dst, dst_ref=dst, send_sem=send_sem.at[0], recv_sem=sem,
            device_id=(mate, t), device_id_type=MESH,
        ).wait_recv()

    def block_of(group):
        return pl.ds(pl.multiple_of(group * feats, feats), feats)

    for other in chips:
        for c in range(CORES):
            group = other * CORES + c
            send(rows.at[t, :, block_of(group)], cols_ref.at[chip, core, t], cross_sem.at[chip, core], (group, t))
    for peer in lines + sides:
        send(rows.at[t], rows.at[t], rows_sem.at[t], (dp, peer))

    loads[1].wait()
    loads[2].wait()
    g = gate[...].astype(jnp.float32)
    u = upper[...].astype(jnp.float32)
    hidden_ref[chip, core] = (g * jax.nn.sigmoid(g) * u).astype(jnp.bfloat16)
    mine = hidden_ref.at[chip, core]
    for other in chips:
        send(mine, mine, hidden_sem.at[chip, core], (other * CORES + core, t))
    send(mine, mine, hidden_sem.at[chip, core], (mate, t))

    for other in chips:
        for c in range(CORES):
            arrived(cols_ref.at[other, c, t], cross_sem.at[other, c])
        block = cols_ref.at[other, :, t]
        for peer in lines + sides:
            send(block, block, line_sem.at[other, t], (dp, peer))

    for source in lines:
        arrived(rows.at[source], rows_sem.at[source])
        for side in sides:
            send(rows.at[source], rows.at[source], rows_sem.at[source], (dp, side))
    for source in lines:
        for other in chips:
            block = cols_ref.at[other, :, source]
            arrived(block, line_sem.at[other, source])
            for side in sides:
                send(block, block, line_sem.at[other, source], (dp, side))

    for other in chips:
        block = hidden_ref.at[other, core]
        arrived(block, hidden_sem.at[other, core])
        send(block, block, hidden_sem.at[other, core], (mate, t))

    from_sides = [
        step * inner + lax.rem(b + d, inner)
        for step in range(outer) for d in range(1, inner)
    ]
    for source in from_sides:
        arrived(rows.at[source], rows_sem.at[source])
    send(rows.at[:, :, block_of(mate)], cols_ref.at[chip, core], pair_sem.at[0], (mate, t))
    keep = pltpu.make_async_copy(rows.at[:, :, block_of(dp)], cols_ref.at[chip, core], load_sem.at[3])
    keep.start()

    left[...] = rows[...].astype(jnp.float32).reshape(n_t * depth, -1).astype(jnp.bfloat16)
    start = 0
    for k, width in enumerate(widths):
        weight_loads[k].wait()
        span = pl.ds(start, width)
        grad_ref[:, span] = lax.dot_general(
            left[...], weight[span, :], (((1,), (1,)), ((), ())), preferred_element_type=jnp.float32
        )
        start += width

    for source in from_sides:
        for other in chips:
            arrived(cols_ref.at[other, :, source], line_sem.at[other, source])
    for other in chips + [chip]:
        arrived(hidden_ref.at[other, 1 - core], hidden_sem.at[other, 1 - core])
    arrived(cols_ref.at[chip, 1 - core], pair_sem.at[0])
    keep.wait()
    for copy in sent:
        copy.wait_send()


def finish_kernel(cols_ref, hidden_ref, grad_ref, gate_ref, up_ref, weight_out, gate_out, up_out):
    weight_out[...] = lax.dot_general(
        hidden_ref[...], cols_ref[...], (((0,), (0,)), ((), ())), preferred_element_type=jnp.float32
    )
    grad = grad_ref[...]
    gate = gate_ref[...].astype(jnp.float32)
    upper = up_ref[...].astype(jnp.float32)
    sig = jax.nn.sigmoid(gate)
    up_out[...] = (grad * (gate * sig)).astype(jnp.bfloat16)
    gate_out[...] = (grad * upper * sig * (1.0 + gate * (1.0 - sig))).astype(jnp.bfloat16)


def body(n_dp, n_t, grad_out, gate_pre, up_pre, down_weight):
    depth, model = grad_out.shape
    group, wide = gate_pre.shape
    feats = model // n_dp
    n_chip = n_dp // CORES
    outer = 4 if n_t % 4 == 0 else 1
    inner = n_t // outer
    step = 512
    widths = [min(step, wide - start) for start in range(0, wide, step)]
    n_send = (
        (n_chip - 1) * CORES + (outer + inner - 2) * n_chip + n_chip
        + (outer - 1) * (inner - 1) * n_chip + n_chip + 1
    )
    anywhere = pl.BlockSpec(memory_space=pl.ANY)
    vmem = pl.BlockSpec(memory_space=pltpu.VMEM)
    dma = pltpu.SemaphoreType.DMA
    cols, hidden, grad = pl.pallas_call(
        functools.partial(gather_kernel, n_dp, n_t, outer, widths),
        out_shape=[
            jax.ShapeDtypeStruct((n_chip, CORES, n_t, depth, feats), jnp.bfloat16),
            jax.ShapeDtypeStruct((n_chip, CORES, group, wide), jnp.bfloat16),
            jax.ShapeDtypeStruct((group, wide), jnp.float32),
        ],
        in_specs=[anywhere] * 4,
        out_specs=[vmem] * 3,
        scratch_shapes=[
            pltpu.VMEM((n_t, depth, model), jnp.bfloat16),
            pltpu.VMEM((group, wide), jnp.bfloat16),
            pltpu.VMEM((group, wide), jnp.bfloat16),
            pltpu.VMEM((wide, model), jnp.bfloat16),
            pltpu.VMEM((group, model), jnp.bfloat16),
            dma((4,)),
            dma((len(widths),)),
            dma((n_send,)),
            dma((n_t,)),
            dma((n_chip, CORES)),
            dma((n_chip, n_t)),
            dma((n_chip, CORES)),
            dma((1,)),
        ],
        compiler_params=pltpu.CompilerParams(
            collective_id=0, has_side_effects=True, vmem_limit_bytes=48 * 1024 * 1024
        ),
    )(grad_out, gate_pre, up_pre, down_weight.T)
    cols = cols.reshape(n_dp * group, feats)
    hidden = hidden.reshape(n_dp * group, wide)

    tile = 256
    tiles = pl.BlockSpec((group, tile), lambda i: (0, i))
    turned, grad_gate, grad_up = pl.pallas_call(
        finish_kernel,
        grid=(pl.cdiv(wide, tile),),
        out_shape=[
            jax.ShapeDtypeStruct((wide, feats), jnp.float32),
            jax.ShapeDtypeStruct((group, wide), jnp.bfloat16),
            jax.ShapeDtypeStruct((group, wide), jnp.bfloat16),
        ],
        in_specs=[
            pl.BlockSpec((n_dp * group, feats), lambda i: (0, 0)),
            pl.BlockSpec((n_dp * group, tile), lambda i: (0, i)),
            tiles, tiles, tiles,
        ],
        out_specs=[pl.BlockSpec((tile, feats), lambda i: (i, 0)), tiles, tiles],
        compiler_params=pltpu.CompilerParams(vmem_limit_bytes=48 * 1024 * 1024),
    )(cols, hidden, grad, gate_pre, up_pre)
    return turned.T, grad_gate, grad_up


def solution(mesh):
    in_specs = (P(("dp", "tensor"), None), P("dp", "tensor"), P("dp", "tensor"), P(None, "tensor"))
    out_specs = (P("dp", "tensor"), P("dp", "tensor"), P("dp", "tensor"))
    fn = functools.partial(body, mesh.shape["dp"], mesh.shape["tensor"])
    return jax.shard_map(fn, mesh=mesh, in_specs=in_specs, out_specs=out_specs, check_vma=False)
```

```python
import functools

import jax
import jax.numpy as jnp
from jax import lax
from jax.experimental import pallas as pl
from jax.experimental.pallas import tpu as pltpu
from jax.sharding import PartitionSpec as P

MESH = pl.DeviceIdType.MESH
CORES = 2
PARTS = 2
VMEM = 67043328


def gather_kernel(
    n_dp, n_t, outer, widths,
    go_hbm, gate_hbm, up_hbm, weight_hbm,
    cols_ref, hidden_ref, grad_ref,
    rows, gate, upper, weight, left,
    load_sem, weight_sem, send_sem,
    rows_sem, cross_sem, line_sem, hidden_sem, pair_sem,
):
    inner = n_t // outer
    n_chip = n_dp // CORES
    depth = go_hbm.shape[0]
    feats = cols_ref.shape[-1]
    share = go_hbm.shape[1] // PARTS
    parts = [pl.ds(h * share, share) for h in range(PARTS)]
    dp, t = lax.axis_index("dp"), lax.axis_index("tensor")
    chip, core = dp // CORES, dp % CORES
    mate = chip * CORES + (1 - core)
    a, b = t // inner, t % inner
    chips = [lax.rem(chip + d, n_chip) for d in range(1, n_chip)]
    lines = [lax.rem(a + d, outer) * inner + b for d in range(1, outer)]
    sides = [a * inner + lax.rem(b + d, inner) for d in range(1, inner)]

    loads = [
        pltpu.make_async_copy(go_hbm, rows.at[t], load_sem.at[0]),
        pltpu.make_async_copy(gate_hbm, gate, load_sem.at[1]),
        pltpu.make_async_copy(up_hbm, upper, load_sem.at[2]),
    ]
    for load in loads:
        load.start()
    weight_loads = []
    start = 0
    for k, width in enumerate(widths):
        span = pl.ds(start, width)
        weight_loads.append(pltpu.make_async_copy(weight_hbm.at[span], weight.at[span], weight_sem.at[k]))
        weight_loads[-1].start()
        start += width

    barrier = pltpu.get_barrier_semaphore()
    peers = [(lax.rem(dp + d, n_dp), t) for d in range(1, n_dp)]
    peers += [(dp, other) for other in lines + sides]
    for peer in peers:
        pl.semaphore_signal(barrier, inc=1, device_id=peer, device_id_type=MESH)
    loads[0].wait()
    pl.semaphore_wait(barrier, len(peers))

    sent = []

    def send(src, dst, sem, peer):
        copy = pltpu.make_async_remote_copy(
            src_ref=src, dst_ref=dst, send_sem=send_sem.at[len(sent)], recv_sem=sem,
            device_id=peer, device_id_type=MESH,
        )
        copy.start()
        sent.append(copy)

    def arrived(dst, sem):
        pltpu.make_async_remote_copy(
            src_ref=dst, dst_ref=dst, send_sem=send_sem.at[0], recv_sem=sem,
            device_id=(mate, t), device_id_type=MESH,
        ).wait_recv()

    def block_of(group):
        return pl.ds(pl.multiple_of(group * feats, feats), feats)

    for other in chips:
        for c in range(CORES):
            group = other * CORES + c
            send(rows.at[t, :, block_of(group)], cols_ref.at[chip, core, t], cross_sem.at[chip, core], (group, t))
    for h, part in enumerate(parts):
        mine = rows.at[t, :, part]
        for peer in lines + sides:
            send(mine, mine, rows_sem.at[h, t], (dp, peer))

    loads[1].wait()
    loads[2].wait()
    g = gate[...].astype(jnp.float32)
    u = upper[...].astype(jnp.float32)
    hidden_ref[chip, core] = (g * jax.nn.sigmoid(g) * u).astype(jnp.bfloat16)
    mine = hidden_ref.at[chip, core]
    for other in chips:
        send(mine, mine, hidden_sem.at[chip, core], (other * CORES + core, t))
    send(mine, mine, hidden_sem.at[chip, core], (mate, t))

    for other in chips:
        for c in range(CORES):
            arrived(cols_ref.at[other, c, t], cross_sem.at[other, c])
        block = cols_ref.at[other, :, t]
        for peer in lines + sides:
            send(block, block, line_sem.at[other, t], (dp, peer))

    for h, part in enumerate(parts):
        for source in lines:
            block = rows.at[source, :, part]
            arrived(block, rows_sem.at[h, source])
            for side in sides:
                send(block, block, rows_sem.at[h, source], (dp, side))

    for other in chips:
        block = hidden_ref.at[other, core]
        arrived(block, hidden_sem.at[other, core])
        send(block, block, hidden_sem.at[other, core], (mate, t))

    def pass_on(source):
        for other in chips:
            block = cols_ref.at[other, :, source]
            arrived(block, line_sem.at[other, source])
            for side in sides:
                send(block, block, line_sem.at[other, source], (dp, side))

    from_sides = [
        step * inner + lax.rem(b + d, inner)
        for step in range(outer) for d in range(1, inner)
    ]
    waiting = list(lines)
    for h, part in enumerate(parts):
        for source in from_sides:
            arrived(rows.at[source, :, part], rows_sem.at[h, source])
        if h == PARTS - 1:
            send(rows.at[:, :, block_of(mate)], cols_ref.at[chip, core], pair_sem.at[0], (mate, t))
            keep = pltpu.make_async_copy(rows.at[:, :, block_of(dp)], cols_ref.at[chip, core], load_sem.at[3])
            keep.start()
        left[:, part] = rows[:, :, part].astype(jnp.float32).reshape(n_t * depth, share).astype(jnp.bfloat16)
        start = 0
        for k, width in enumerate(widths):
            if h == 0:
                weight_loads[k].wait()
            span = pl.ds(start, width)
            term = lax.dot_general(
                left[:, part], weight[span, part], (((1,), (1,)), ((), ())), preferred_element_type=jnp.float32
            )
            grad_ref[:, span] = term if h == 0 else grad_ref[:, span] + term
            start += width
            if waiting:
                pass_on(waiting.pop(0))
    while waiting:
        pass_on(waiting.pop(0))

    for source in from_sides:
        for other in chips:
            arrived(cols_ref.at[other, :, source], line_sem.at[other, source])
    for other in chips + [chip]:
        arrived(hidden_ref.at[other, 1 - core], hidden_sem.at[other, 1 - core])
    arrived(cols_ref.at[chip, 1 - core], pair_sem.at[0])
    keep.wait()
    for copy in sent:
        copy.wait_send()


def finish_kernel(cols_ref, hidden_ref, grad_ref, gate_ref, up_ref, weight_out, gate_out, up_out):
    weight_out[...] = lax.dot_general(
        hidden_ref[...], cols_ref[...], (((0,), (0,)), ((), ())), preferred_element_type=jnp.float32
    )
    grad = grad_ref[...]
    gate = gate_ref[...].astype(jnp.float32)
    upper = up_ref[...].astype(jnp.float32)
    sig = jax.nn.sigmoid(gate)
    up_out[...] = (grad * (gate * sig)).astype(jnp.bfloat16)
    gate_out[...] = (grad * upper * sig * (1.0 + gate * (1.0 - sig))).astype(jnp.bfloat16)


def body(n_dp, n_t, grad_out, gate_pre, up_pre, down_weight):
    depth, model = grad_out.shape
    group, wide = gate_pre.shape
    feats = model // n_dp
    n_chip = n_dp // CORES
    outer = 4 if n_t % 4 == 0 else 1
    inner = n_t // outer
    step = 512
    widths = [min(step, wide - start) for start in range(0, wide, step)]
    n_send = (
        (n_chip - 1) * CORES + (outer * inner - 1) * (n_chip - 1 + PARTS) + 2 * n_chip
    )
    lanes = pl.cdiv(wide, 128) * 128
    results = 2 * n_dp * group * (feats + lanes) + 4 * group * lanes
    anywhere = pl.BlockSpec(memory_space=pltpu.HBM)
    vmem = pl.BlockSpec(memory_space=pltpu.VMEM)
    dma = pltpu.SemaphoreType.DMA
    cols, hidden, grad = pl.pallas_call(
        functools.partial(gather_kernel, n_dp, n_t, outer, widths),
        out_shape=[
            jax.ShapeDtypeStruct((n_chip, CORES, n_t, depth, feats), jnp.bfloat16),
            jax.ShapeDtypeStruct((n_chip, CORES, group, wide), jnp.bfloat16),
            jax.ShapeDtypeStruct((group, wide), jnp.float32),
        ],
        in_specs=[anywhere] * 4,
        out_specs=[vmem] * 3,
        scratch_shapes=[
            pltpu.VMEM((n_t, depth, model), jnp.bfloat16),
            pltpu.VMEM((group, wide), jnp.bfloat16),
            pltpu.VMEM((group, wide), jnp.bfloat16),
            pltpu.VMEM((wide, model), jnp.bfloat16),
            pltpu.VMEM((group, model), jnp.bfloat16),
            dma((4,)),
            dma((len(widths),)),
            dma((n_send,)),
            dma((PARTS, n_t)),
            dma((n_chip, CORES)),
            dma((n_chip, n_t)),
            dma((n_chip, CORES)),
            dma((1,)),
        ],
        compiler_params=pltpu.CompilerParams(
            collective_id=0, has_side_effects=True, vmem_limit_bytes=VMEM - results - 16 * 1024
        ),
    )(grad_out, gate_pre, up_pre, down_weight.T)
    cols = cols.reshape(n_dp * group, feats)
    hidden = hidden.reshape(n_dp * group, wide)

    tile = 512
    tiles = pl.BlockSpec((group, tile), lambda i: (0, i))
    turned, grad_gate, grad_up = pl.pallas_call(
        finish_kernel,
        grid=(pl.cdiv(wide, tile),),
        out_shape=[
            jax.ShapeDtypeStruct((wide, feats), jnp.float32),
            jax.ShapeDtypeStruct((group, wide), jnp.bfloat16),
            jax.ShapeDtypeStruct((group, wide), jnp.bfloat16),
        ],
        in_specs=[
            pl.BlockSpec((n_dp * group, feats), lambda i: (0, 0)),
            pl.BlockSpec((n_dp * group, tile), lambda i: (0, i)),
            tiles, tiles, tiles,
        ],
        out_specs=[pl.BlockSpec((tile, feats), lambda i: (i, 0)), tiles, tiles],
        compiler_params=pltpu.CompilerParams(vmem_limit_bytes=VMEM - results - 16 * 1024),
    )(cols, hidden, grad, gate_pre, up_pre)
    return turned.T, grad_gate, grad_up


def solution(mesh):
    in_specs = (P(("dp", "tensor"), None), P("dp", "tensor"), P("dp", "tensor"), P(None, "tensor"))
    out_specs = (P("dp", "tensor"), P("dp", "tensor"), P("dp", "tensor"))
    fn = functools.partial(body, mesh.shape["dp"], mesh.shape["tensor"])
    return jax.shard_map(fn, mesh=mesh, in_specs=in_specs, out_specs=out_specs, check_vma=False)
```
